512 devices in a mesh: files: 128 (over y, z, core), rep: 4 (over x).
Axes of the slice: x: 4, y: 8, z: 8, core: 2. Of those that a mesh axis runs over, the one named last changes fastest.
Arguments:
- tile_id: int32 [2097152], P(('files', 'rep')), may hold values from 0 to 127, as said below
- pix_row: int32 [2097152], P(('files', 'rep')), may hold values from 0 to 31
- pix_col: int32 [2097152], P(('files', 'rep')), may hold values from 0 to 127
- point_value: bfloat16 [2097152], P(('files', 'rep')), may hold values from -6 to 6
Outputs:
- tile_sums: float32 [128, 32, 128], P('files', 'rep')
The draws below stay inside these ranges and needn't reach their ends.
Inputs may be any that keep to these rules, and one draw needn't show every extreme that they name: `tile_id`: of the points of one device, at most 128 lie in tiles of one file group (tile id modulo 128), and on every device some group holds exactly 128 of them.
All inputs are finite; a program needn't handle non-finite values.
Results may differ from the reference program's by a relative error of at most 0.0003.
Values sent between devices are 32-bit elements; how exact they have to be, the bound alone decides.
A program may use at most 64 MiB of HBM per device.

```python
import jax
import jax.numpy as jnp

TC = 128
TR = 32
PTS_DEV = 4096
TILES = 128
TILE_OWN = 1
CAP = 128
POINTS = 2097152
N_FILES = 128
N_REP = 4


def draw_tile_id(key, part):
    device_count = POINTS // PTS_DEV
    tier_most = N_FILES // 8
    middle_low = max(1, CAP // 4)
    middle_high = max(middle_low, CAP // 2)

    def one_device(device_key):
        key_order = jax.random.fold_in(device_key, 1)
        key_local = jax.random.fold_in(device_key, 2)
        key_mixing = jax.random.fold_in(device_key, 3)
        key_heavy = jax.random.fold_in(device_key, 4)
        key_middle = jax.random.fold_in(device_key, 5)
        key_size = jax.random.fold_in(device_key, 6)
        owner_order = jax.random.permutation(key_order, N_FILES)
        heavy_count = jax.random.randint(key_heavy, (), 1, tier_most + 1)
        middle_count = jax.random.randint(key_middle, (), 0, tier_most + 1)
        middle_size = jax.random.randint(key_size, (), middle_low, middle_high + 1)
        slot_index = jnp.arange(PTS_DEV, dtype=jnp.int32)
        heavy_end = heavy_count * CAP
        middle_end = heavy_end + middle_count * middle_size
        rest_owners = N_FILES - heavy_count - middle_count
        rank_heavy = slot_index // CAP
        rank_middle = heavy_count + (slot_index - heavy_end) // middle_size
        rank_rest = heavy_count + middle_count + (slot_index - middle_end) % rest_owners
        pick_rank = jnp.where(slot_index < heavy_end, rank_heavy, jnp.where(slot_index < middle_end, rank_middle, rank_rest))
        pick_rank = jnp.clip(pick_rank, 0, N_FILES - 1).astype(jnp.int32)
        tile_owner = owner_order[pick_rank]
        tile_local = jax.random.randint(key_local, (PTS_DEV,), 0, TILE_OWN)
        tile_ids = tile_owner + N_FILES * tile_local
        return jax.random.permutation(key_mixing, tile_ids)
    device_keys = jax.random.split(jax.random.fold_in(key, 11), device_count)
    return jax.vmap(one_device)(device_keys).reshape(POINTS).astype(jnp.int32)


def draw_pix_row(key, part):
    device_count = POINTS // PTS_DEV
    quarter = TR // N_REP

    def one_device(device_key):
        hot_quarter = jax.random.randint(jax.random.fold_in(device_key, 1), (), 0, N_REP)
        hot_share = jax.random.randint(jax.random.fold_in(device_key, 2), (), 3, 8)
        pick_tenth = jax.random.randint(jax.random.fold_in(device_key, 3), (PTS_DEV,), 0, 10)
        inner_row = jax.random.randint(jax.random.fold_in(device_key, 4), (PTS_DEV,), 0, quarter)
        spread_row = jax.random.randint(jax.random.fold_in(device_key, 5), (PTS_DEV,), 0, TR)
        return jnp.where(pick_tenth < hot_share, hot_quarter * quarter + inner_row, spread_row)
    device_keys = jax.random.split(jax.random.fold_in(key, 21), device_count)
    return jax.vmap(one_device)(device_keys).reshape(POINTS).astype(jnp.int32)


def with_ends(values, stream_key, smallest, top_value):
    extent = values.shape
    index_at = [jax.random.randint(jax.random.fold_in(stream_key, axis), (), 0, extent[axis]) for axis in range(len(extent))]
    values = values.at[tuple(index_at)].set(smallest)
    longest = extent.index(max(extent))
    index_at[longest] = (index_at[longest] + 1) % extent[longest]
    return values.at[tuple(index_at)].set(top_value)


def levels(own_key, shape, shards, least, largest):
    loudness = 1.0
    for dim, blocks in shards:
        draws = jax.random.uniform(jax.random.fold_in(jax.random.fold_in(own_key, 6), dim), (blocks,), jnp.float32, least / len(shards), largest / len(shards))
        loudness = loudness * jnp.repeat(jnp.exp(draws), shape[dim] // blocks).reshape((-1,) + (1,) * (len(shape) - 1 - dim))
    return loudness


def centred(key, shape, scale, limit, shards=(), kind=jnp.bfloat16):
    result = jax.random.normal(key, shape, jnp.float32) * scale
    if len(shards) > 0:
        result = levels(key, shape, shards, -0.22, 0.18) * result
    return jnp.clip(result, min=-limit, max=limit).astype(kind)


def setup_inputs(seed: int = 0) -> dict:
    keys = jax.random.split(jax.random.key(seed), 5)
    return {
        "tile_id": draw_tile_id(jax.random.fold_in(keys[4], 71), 0),
        "pix_row": draw_pix_row(jax.random.fold_in(keys[4], 71), 0),
        "pix_col": with_ends(jax.random.randint(keys[2], (POINTS,), 0, TC), jax.random.fold_in(keys[2], 1), 0, TC - 1).astype(jnp.int32),
        "point_value": centred(keys[3], (POINTS,), 1.0, 6.0, ((0, 512),)),
    }


def reference(tile_id, pix_row, pix_col, point_value):
    tile_owner = tile_id % N_FILES
    tile_local = tile_id // N_FILES
    owned_slot = tile_owner * TILE_OWN + tile_local
    flat_cell = (owned_slot * TR + pix_row) * TC + pix_col
    summed = jax.ops.segment_sum(point_value.astype(jnp.float32), flat_cell.astype(jnp.int32), num_segments=TILES * TR * TC)
    return summed.reshape(TILES, TR, TC)
```

```python
import functools

import jax
import jax.numpy as jnp
from jax import lax
from jax.experimental import pallas as pl
from jax.experimental.pallas import tpu as pltpu
from jax.sharding import PartitionSpec as P

TC = 128
TR = 32
CAP = 128
LANES = 128
SUB = 16
MESH = pl.DeviceIdType.MESH
BF = jnp.bfloat16
F32 = jnp.float32
NT = (((1,), (1,)), ((), ()))


def packed_row(row):
    return jnp.broadcast_to(row, (SUB, LANES)).astype(BF)


def packed_iota(rows):
    count = lax.broadcasted_iota(jnp.int32, (rows // SUB, SUB, LANES), 0) * SUB
    return (count + lax.broadcasted_iota(jnp.int32, (rows // SUB, SUB, LANES), 1)).astype(F32).astype(BF)


def kernel(
    files,
    reps,
    tid_hbm,
    row_hbm,
    col_hbm,
    val_hbm,
    out_ref,
    tid_in,
    row_in,
    col_in,
    val_in,
    points,
    send,
    recv,
    part,
    gathered,
    in_sem,
    send_sem,
    recv_sem,
    part_send_sem,
    part_recv_sem,
):
    f = lax.axis_index("files")
    r = lax.axis_index("rep")
    blocks = tid_in.shape[0]
    quarter = TR // reps

    loads = [
        pltpu.make_async_copy(source, target, in_sem.at[i])
        for i, (source, target) in enumerate(
            ((tid_hbm, tid_in), (row_hbm, row_in), (col_hbm, col_in), (val_hbm, val_in))
        )
    ]
    for load in loads:
        load.start()

    barrier = pltpu.get_barrier_semaphore()

    def greet(k, _):
        peer = lax.rem(f + k, files)
        pl.semaphore_signal(barrier, inc=1, device_id={"files": peer, "rep": r}, device_id_type=MESH)
        return 0

    lax.fori_loop(1, files, greet, 0)
    for k in range(1, reps):
        pl.semaphore_signal(
            barrier, inc=1, device_id={"files": f, "rep": lax.rem(r + k, reps)}, device_id_type=MESH
        )

    for load in loads:
        load.wait()
    points[0] = tid_in[...].astype(F32)
    points[1] = row_in[...].astype(F32)
    points[2] = col_in[...].astype(F32)
    points[3] = val_in[...].astype(F32)

    iota = packed_iota(LANES)
    one, zero = jnp.ones((), BF), jnp.zeros((), BF)

    def tally(b, total):
        tid = packed_row(points[0, pl.ds(b, 1), :])
        return total + jnp.where(iota == tid[None], one, zero)

    total = lax.fori_loop(0, blocks, tally, jnp.zeros((LANES // SUB, SUB, LANES), BF), unroll=8)
    earlier = jnp.where(
        lax.broadcasted_iota(jnp.int32, (LANES, LANES), 0) < lax.broadcasted_iota(jnp.int32, (LANES, LANES), 1),
        1.0,
        0.0,
    ).astype(BF)
    before = jnp.dot(total.reshape(LANES, LANES), earlier, preferred_element_type=F32)
    before = before.astype(BF).reshape(LANES // SUB, SUB, LANES)

    def place(b, carry):
        before, packed = carry
        lefts, rights = [], []
        for half in range(2):
            at = b * 2 + half
            hit = iota == packed_row(points[0, pl.ds(at, 1), :])[None]
            slot = jnp.sum(jnp.where(hit, before, zero), axis=0)
            slot = jnp.sum(slot.astype(F32), axis=0, keepdims=True)
            before = before + jnp.where(hit, one, zero)
            rights.append(jnp.where(iota == packed_row(slot)[None], one, zero).reshape(LANES, LANES))
            lefts.append(
                jnp.concatenate(
                    [
                        jnp.where(hit, packed_row(points[i, pl.ds(at, 1), :])[None], zero).reshape(LANES, LANES)
                        for i in (1, 2, 3)
                    ],
                    axis=0,
                )
            )
        left, right = jnp.concatenate(lefts, axis=1), jnp.concatenate(rights, axis=1)
        return before, packed + lax.dot_general(left, right, NT, preferred_element_type=F32)

    _, packed = lax.fori_loop(
        0, blocks // 2, place, (before, jnp.zeros((3 * LANES, CAP), F32)), unroll=4
    )
    send[:, 0, :] = packed[2 * LANES :][:files]
    send[:, 1, :] = (packed[:LANES] * TC + packed[LANES : 2 * LANES])[:files]

    pl.semaphore_wait(barrier, files - 1 + reps - 1)

    def scatter(k, _):
        peer = lax.rem(f + k, files)
        pltpu.make_async_remote_copy(
            src_ref=send.at[peer],
            dst_ref=recv.at[k],
            send_sem=send_sem,
            recv_sem=recv_sem,
            device_id={"files": peer, "rep": r},
            device_id_type=MESH,
        ).start()
        return 0

    lax.fori_loop(1, files, scatter, 0)
    recv[0] = send[f]
    whole = recv.at[pl.ds(1, files - 1)]
    pltpu.make_async_copy(whole, whole, recv_sem).wait()

    row_iota = packed_iota(TR)

    def raster(s, total):
        lefts, rights = [], []
        for half in range(8):
            block = recv[s * 8 + half]
            cell = block[1:2]
            row = jnp.floor(cell * (1.0 / TC))
            col = cell - row * TC
            rights.append(jnp.where(row_iota == packed_row(row)[None], one, zero).reshape(TR, LANES))
            lefts.append(
                jnp.where(iota == packed_row(col)[None], packed_row(block[0:1])[None], zero).reshape(LANES, LANES)
            )
        left, right = jnp.concatenate(lefts, axis=1), jnp.concatenate(rights, axis=1)
        return total + lax.dot_general(left, right, NT, preferred_element_type=F32)

    tile = lax.fori_loop(0, files // 8, raster, jnp.zeros((TC, TR), F32), unroll=2 if files % 16 == 0 else 1)
    part[...] = tile.T.reshape(reps, quarter, TC)

    for k in range(1, reps):
        peer = lax.rem(r + k, reps)
        pltpu.make_async_remote_copy(
            src_ref=part.at[peer],
            dst_ref=gathered.at[k - 1],
            send_sem=part_send_sem,
            recv_sem=part_recv_sem,
            device_id={"files": f, "rep": peer},
            device_id_type=MESH,
        ).start()
    pltpu.make_async_copy(gathered, gathered, part_recv_sem).wait()
    out = part[r]
    for k in range(reps - 1):
        out = out + gathered[k]
    out_ref[...] = out

    sent = send.at[pl.ds(1, files - 1)]
    pltpu.make_async_copy(sent, sent, send_sem).wait()
    pltpu.make_async_copy(gathered, gathered, part_send_sem).wait()


def solution(mesh):
    files, reps = mesh.shape["files"], mesh.shape["rep"]

    def per_device(tile_id, pix_row, pix_col, point_value):
        count = tile_id.shape[0]
        blocks = count // LANES
        shaped = [a.reshape(blocks, LANES) for a in (tile_id, pix_row, pix_col, point_value)]
        out = pl.pallas_call(
            functools.partial(kernel, files, reps),
            out_shape=jax.ShapeDtypeStruct((TR // reps, TC), F32),
            in_specs=[pl.BlockSpec(memory_space=pl.ANY)] * 4,
            out_specs=pl.BlockSpec(memory_space=pltpu.VMEM),
            scratch_shapes=[
                pltpu.VMEM((blocks, LANES), jnp.int32),
                pltpu.VMEM((blocks, LANES), jnp.int32),
                pltpu.VMEM((blocks, LANES), jnp.int32),
                pltpu.VMEM((blocks, LANES), BF),
                pltpu.VMEM((4, blocks, LANES), F32),
                pltpu.VMEM((files, 2, CAP), F32),
                pltpu.VMEM((files, 2, CAP), F32),
                pltpu.VMEM((reps, TR // reps, TC), F32),
                pltpu.VMEM((reps - 1, TR // reps, TC), F32),
                pltpu.SemaphoreType.DMA((4,)),
                pltpu.SemaphoreType.DMA,
                pltpu.SemaphoreType.DMA,
                pltpu.SemaphoreType.DMA,
                pltpu.SemaphoreType.DMA,
            ],
            compiler_params=pltpu.CompilerParams(collective_id=0, has_side_effects=True),
        )(*shaped)
        return out[None]

    spec = P(("files", "rep"))
    return jax.shard_map(
        per_device,
        mesh=mesh,
        in_specs=(spec, spec, spec, spec),
        out_specs=P("files", "rep", None),
        check_vma=False,
    )
```

```python
import functools

import jax
import jax.numpy as jnp
from jax import lax
from jax.experimental import pallas as pl
from jax.experimental.pallas import tpu as pltpu
from jax.sharding import PartitionSpec as P

TC = 128
TR = 32
CAP = 128
LANES = 128
SUB = 16
DEPTH = 8
RASTER = 8
MESH = pl.DeviceIdType.MESH
BF = jnp.bfloat16
F32 = jnp.float32
NT = (((1,), (1,)), ((), ()))


def packed_row(row):
    return jnp.broadcast_to(row, (SUB, LANES)).astype(BF)


def packed_iota(rows):
    count = lax.broadcasted_iota(jnp.int32, (rows // SUB, SUB, LANES), 0) * SUB
    return (count + lax.broadcasted_iota(jnp.int32, (rows // SUB, SUB, LANES), 1)).astype(F32).astype(BF)


def kernel(
    files,
    reps,
    tid_hbm,
    row_hbm,
    col_hbm,
    val_hbm,
    out_ref,
    tid_in,
    row_in,
    col_in,
    val_in,
    points,
    send,
    recv,
    part,
    gathered,
    in_sem,
    send_sem,
    recv_sem,
    above,
    part_send_sem,
    part_recv_sem,
):
    f = lax.axis_index("files")
    r = lax.axis_index("rep")
    depth, line = recv.shape[:2]
    z = lax.rem(f // 2, depth)
    i = f // (2 * depth) * 2 + lax.rem(f, 2)

    def file_at(place, level):
        return (place // 2 * depth + level) * 2 + lax.rem(place, 2)

    blocks = tid_in.shape[0]
    quarter = TR // reps

    loads = [
        pltpu.make_async_copy(source, target, in_sem.at[i])
        for i, (source, target) in enumerate(
            ((tid_hbm, tid_in), (row_hbm, row_in), (col_hbm, col_in), (val_hbm, val_in))
        )
    ]
    for load in loads:
        load.start()

    barrier = pltpu.get_barrier_semaphore()
    for j in range(1, line):
        peer = lax.rem(i + j, line)
        pl.semaphore_signal(
            barrier, inc=1, device_id={"files": file_at(peer, z), "rep": r}, device_id_type=MESH
        )
    for k in range(1, reps):
        pl.semaphore_signal(
            barrier, inc=1, device_id={"files": f, "rep": lax.rem(r + k, reps)}, device_id_type=MESH
        )

    for load in loads:
        load.wait()
    points[0] = tid_in[...].astype(F32)
    points[1] = row_in[...].astype(F32)
    points[2] = col_in[...].astype(F32)
    points[3] = val_in[...].astype(F32)

    iota = packed_iota(LANES)
    one, zero = jnp.ones((), BF), jnp.zeros((), BF)

    def tally(b, total):
        tid = packed_row(points[0, pl.ds(b, 1), :])
        return total + jnp.where(iota == tid[None], one, zero)

    total = lax.fori_loop(0, blocks, tally, jnp.zeros((LANES // SUB, SUB, LANES), BF), unroll=8)
    earlier = jnp.where(
        lax.broadcasted_iota(jnp.int32, (LANES, LANES), 0) < lax.broadcasted_iota(jnp.int32, (LANES, LANES), 1),
        1.0,
        0.0,
    ).astype(BF)
    before = jnp.dot(total.reshape(LANES, LANES), earlier, preferred_element_type=F32)
    before = before.astype(BF).reshape(LANES // SUB, SUB, LANES)

    def place(b, carry):
        before, packed = carry
        lefts, rights = [], []
        for half in range(2):
            at = b * 2 + half
            hit = iota == packed_row(points[0, pl.ds(at, 1), :])[None]
            slot = jnp.sum(jnp.where(hit, before, zero), axis=0)
            slot = jnp.sum(slot.astype(F32), axis=0, keepdims=True)
            before = before + jnp.where(hit, one, zero)
            rights.append(jnp.where(iota == packed_row(slot)[None], one, zero).reshape(LANES, LANES))
            lefts.append(
                jnp.concatenate(
                    [
                        jnp.where(hit, packed_row(points[i, pl.ds(at, 1), :])[None], zero).reshape(LANES, LANES)
                        for i in (1, 2, 3)
                    ],
                    axis=0,
                )
            )
        left, right = jnp.concatenate(lefts, axis=1), jnp.concatenate(rights, axis=1)
        return before, packed + lax.dot_general(left, right, NT, preferred_element_type=F32)

    _, packed = lax.fori_loop(
        0, blocks // 2, place, (before, jnp.zeros((3 * LANES, CAP), F32)), unroll=4
    )
    send[:, 0, :] = packed[2 * LANES :][:files]
    send[:, 1, :] = (packed[:LANES] * TC + packed[LANES : 2 * LANES])[:files]

    own = pltpu.make_async_copy(send.at[f], recv.at[z, i], recv_sem.at[z])
    own.start()

    def scatter(level, first):
        def one_peer(j, _):
            peer = file_at(lax.rem(i + j, line), level)
            pltpu.make_async_remote_copy(
                src_ref=send.at[peer],
                dst_ref=recv.at[z, i],
                send_sem=send_sem,
                recv_sem=recv_sem.at[z],
                device_id={"files": peer, "rep": r},
                device_id_type=MESH,
            ).start()
            return 0

        lax.fori_loop(first, line, one_peer, 0)

    pl.semaphore_wait(barrier, line - 1 + reps - 1 + jnp.minimum(z, 1))

    @pl.when(z < depth - 1)
    def _():
        pl.semaphore_signal(
            barrier, inc=1, device_id={"files": file_at(i, z + 1), "rep": r}, device_id_type=MESH
        )

    def lower(level, _):
        scatter(level, 0)
        return 0

    def announce(level, _):
        pl.semaphore_signal(
            above.at[z], inc=1, device_id={"files": file_at(i, level), "rep": r}, device_id_type=MESH
        )
        return 0

    lax.fori_loop(0, z, announce, 0)
    lax.fori_loop(0, z, lower, 0)
    scatter(z, 1)

    def upper(level, _):
        pl.semaphore_wait(above.at[level], 1)
        scatter(level, 0)
        return 0

    lax.fori_loop(z + 1, depth, upper, 0)

    row_iota = packed_iota(TR)

    def raster(level, total):
        landed = recv.at[level]
        pltpu.make_async_copy(landed, landed, recv_sem.at[level]).wait()
        for group in range(0, line, RASTER):
            lefts, rights = [], []
            for source in range(group, min(group + RASTER, line)):
                block = recv[level, source]
                cell = block[1:2]
                row = jnp.floor(cell * (1.0 / TC))
                col = cell - row * TC
                rights.append(jnp.where(row_iota == packed_row(row)[None], one, zero).reshape(TR, LANES))
                lefts.append(
                    jnp.where(iota == packed_row(col)[None], packed_row(block[0:1])[None], zero).reshape(LANES, LANES)
                )
            left, right = jnp.concatenate(lefts, axis=1), jnp.concatenate(rights, axis=1)
            total = total + lax.dot_general(left, right, NT, preferred_element_type=F32)
        return total

    tile = lax.fori_loop(0, depth, raster, jnp.zeros((TC, TR), F32))
    part[...] = tile.T.reshape(reps, quarter, TC)

    for k in range(1, reps):
        peer = lax.rem(r + k, reps)
        pltpu.make_async_remote_copy(
            src_ref=part.at[peer],
            dst_ref=gathered.at[k - 1],
            send_sem=part_send_sem,
            recv_sem=part_recv_sem,
            device_id={"files": f, "rep": peer},
            device_id_type=MESH,
        ).start()
    pltpu.make_async_copy(gathered, gathered, part_recv_sem).wait()
    out = part[r]
    for k in range(reps - 1):
        out = out + gathered[k]
    out_ref[...] = out

    sent = send.at[pl.ds(0, files - 1)]
    pltpu.make_async_copy(sent, sent, send_sem).wait()
    pltpu.make_async_copy(gathered, gathered, part_send_sem).wait()


def solution(mesh):
    files, reps = mesh.shape["files"], mesh.shape["rep"]
    depth = DEPTH if files % (2 * DEPTH) == 0 else 2

    def per_device(tile_id, pix_row, pix_col, point_value):
        count = tile_id.shape[0]
        blocks = count // LANES
        shaped = [a.reshape(blocks, LANES) for a in (tile_id, pix_row, pix_col, point_value)]
        out = pl.pallas_call(
            functools.partial(kernel, files, reps),
            out_shape=jax.ShapeDtypeStruct((TR // reps, TC), F32),
            in_specs=[pl.BlockSpec(memory_space=pl.ANY)] * 4,
            out_specs=pl.BlockSpec(memory_space=pltpu.VMEM),
            scratch_shapes=[
                pltpu.VMEM((blocks, LANES), jnp.int32),
                pltpu.VMEM((blocks, LANES), jnp.int32),
                pltpu.VMEM((blocks, LANES), jnp.int32),
                pltpu.VMEM((blocks, LANES), BF),
                pltpu.VMEM((4, blocks, LANES), F32),
                pltpu.VMEM((files, 2, CAP), F32),
                pltpu.VMEM((depth, files // depth, 2, CAP), F32),
                pltpu.VMEM((reps, TR // reps, TC), F32),
                pltpu.VMEM((reps - 1, TR // reps, TC), F32),
                pltpu.SemaphoreType.DMA((4,)),
                pltpu.SemaphoreType.DMA,
                pltpu.SemaphoreType.DMA((depth,)),
                pltpu.SemaphoreType.REGULAR((depth,)),
                pltpu.SemaphoreType.DMA,
                pltpu.SemaphoreType.DMA,
            ],
            compiler_params=pltpu.CompilerParams(collective_id=0, has_side_effects=True),
        )(*shaped)
        return out[None]

    spec = P(("files", "rep"))
    return jax.shard_map(
        per_device,
        mesh=mesh,
        in_specs=(spec, spec, spec, spec),
        out_specs=P("files", "rep", None),
        check_vma=False,
    )
```

```python
import functools

import jax
import jax.numpy as jnp
from jax import lax
from jax.experimental import pallas as pl
from jax.experimental.pallas import tpu as pltpu
from jax.sharding import PartitionSpec as P

TC = 128
TR = 32
CAP = 128
LANES = 128
SUB = 16
DEPTH = 8
RASTER = 8
GROUP = 32
VMEM = 8 << 20
MESH = pl.DeviceIdType.MESH
BF = jnp.bfloat16
F32 = jnp.float32
NT = (((1,), (1,)), ((), ()))


def packed_row(row):
    return jnp.broadcast_to(row, (SUB, LANES)).astype(BF)


def packed_iota(rows):
    count = lax.broadcasted_iota(jnp.int32, (rows // SUB, SUB, LANES), 0) * SUB
    return (count + lax.broadcasted_iota(jnp.int32, (rows // SUB, SUB, LANES), 1)).astype(F32).astype(BF)


def kernel(
    files,
    reps,
    tid_hbm,
    row_hbm,
    col_hbm,
    val_hbm,
    out_ref,
    ids_in,
    val_in,
    points,
    send,
    recv,
    part,
    gathered,
    in_sem,
    send_sem,
    recv_sem,
    above,
    part_send_sem,
    part_recv_sem,
):
    f = lax.axis_index("files")
    r = lax.axis_index("rep")
    depth, line = recv.shape[:2]
    z = lax.rem(f // 2, depth)
    i = f // (2 * depth) * 2 + lax.rem(f, 2)

    def file_at(place, level):
        return (place // 2 * depth + level) * 2 + lax.rem(place, 2)

    blocks = val_in.shape[0]
    quarter = TR // reps

    loads = [
        pltpu.make_async_copy(tid_hbm, ids_in.at[0], in_sem.at[0]),
        pltpu.make_async_copy(row_hbm, ids_in.at[1], in_sem.at[0]),
        pltpu.make_async_copy(col_hbm, ids_in.at[2], in_sem.at[0]),
        pltpu.make_async_copy(val_hbm, val_in, in_sem.at[1]),
    ]
    for load in loads:
        load.start()

    barrier = pltpu.get_barrier_semaphore()
    for j in range(1, line):
        peer = lax.rem(i + j, line)
        pl.semaphore_signal(
            barrier, inc=1, device_id={"files": file_at(peer, z), "rep": r}, device_id_type=MESH
        )
    for k in range(1, reps):
        pl.semaphore_signal(
            barrier, inc=1, device_id={"files": f, "rep": lax.rem(r + k, reps)}, device_id_type=MESH
        )

    pltpu.make_async_copy(ids_in, ids_in, in_sem.at[0]).wait()
    loads[3].wait()
    row = ids_in[1]
    power = jnp.left_shift(1, row & 15).astype(F32) * jnp.where(row >= 16, 65536.0, 1.0)
    points[0] = ids_in[0].astype(F32)
    points[1] = (ids_in[2] + TC).astype(F32) * power
    points[2] = val_in[...].astype(F32)

    iota = packed_iota(LANES)
    one, zero = jnp.ones((), BF), jnp.zeros((), BF)

    def tally(b, total):
        tid = packed_row(points[0, pl.ds(b, 1), :])
        return total + jnp.where(iota == tid[None], one, zero)

    total = lax.fori_loop(0, blocks, tally, jnp.zeros((LANES // SUB, SUB, LANES), BF), unroll=8)
    earlier = jnp.where(
        lax.broadcasted_iota(jnp.int32, (LANES, LANES), 0) < lax.broadcasted_iota(jnp.int32, (LANES, LANES), 1),
        1.0,
        0.0,
    ).astype(BF)
    before = jnp.dot(total.reshape(LANES, LANES), earlier, preferred_element_type=F32)
    before = before.astype(BF).reshape(LANES // SUB, SUB, LANES)

    def place(b, carry):
        before, packed = carry
        lefts, rights = [], []
        for step in range(group):
            at = b * group + step
            hit = iota == packed_row(points[0, pl.ds(at, 1), :])[None]
            slot = jnp.sum(jnp.where(hit, before, zero), axis=0)
            slot = jnp.sum(slot.astype(F32), axis=0, keepdims=True)
            count = jnp.where(hit, one, zero)
            before = before + count
            lefts.append(count.reshape(LANES, LANES))
            here = iota == packed_row(slot)[None]
            rights.append(
                jnp.concatenate(
                    [
                        jnp.where(here, packed_row(points[plane, pl.ds(at, 1), :])[None], zero).reshape(CAP, LANES)
                        for plane in (1, 2)
                    ],
                    axis=0,
                )
            )
        left, right = jnp.concatenate(lefts, axis=1), jnp.concatenate(rights, axis=1)
        return before, packed + lax.dot_general(left, right, NT, preferred_element_type=F32)

    group = min(GROUP, blocks)
    _, packed = lax.fori_loop(0, blocks // group, place, (before, jnp.zeros((LANES, 2 * CAP), F32)))
    code, row = packed[:files, :CAP], jnp.zeros((files, CAP), F32)
    for bit in (16, 8, 4, 2, 1):
        high = code >= 128.0 * 2.0**bit
        code = jnp.where(high, code * 2.0**-bit, code)
        row = row + jnp.where(high, float(bit), 0.0)
    send[pl.ds(0, files, stride=2), :] = packed[:files, CAP:]
    send[pl.ds(1, files, stride=2), :] = row * TC + (code - TC)

    own = pltpu.make_async_copy(send.at[pl.ds(2 * f, 2)], recv.at[z, i], recv_sem.at[z])
    own.start()

    def scatter(level, skip):
        for place in range(line):
            peer = place // 2 * depth * 2 + place % 2 + level * 2

            def start(peer=peer):
                pltpu.make_async_remote_copy(
                    src_ref=send.at[pl.ds(2 * peer, 2)],
                    dst_ref=recv.at[z, i],
                    send_sem=send_sem,
                    recv_sem=recv_sem.at[z],
                    device_id={"files": peer, "rep": r},
                    device_id_type=MESH,
                ).start()

            if skip:
                pl.when(i != place)(start)
            else:
                start()

    pl.semaphore_wait(barrier, line - 1 + reps - 1 + jnp.minimum(z, 1))

    @pl.when(z < depth - 1)
    def _():
        pl.semaphore_signal(
            barrier, inc=1, device_id={"files": file_at(i, z + 1), "rep": r}, device_id_type=MESH
        )

    def lower(level, _):
        scatter(level, False)
        return 0

    def announce(level, _):
        pl.semaphore_signal(
            above.at[z], inc=1, device_id={"files": file_at(i, level), "rep": r}, device_id_type=MESH
        )
        return 0

    lax.fori_loop(0, z, announce, 0)
    lax.fori_loop(0, z, lower, 0)
    scatter(z, True)

    def upper(level, _):
        pl.semaphore_wait(above.at[level], 1)
        scatter(level, False)
        return 0

    lax.fori_loop(z + 1, depth, upper, 0)

    row_iota = packed_iota(TR)

    def raster(level, total):
        landed = recv.at[level]
        pltpu.make_async_copy(landed, landed, recv_sem.at[level]).wait()
        for group in range(0, line, RASTER):
            lefts, rights = [], []
            for source in range(group, min(group + RASTER, line)):
                block = recv[level, source]
                cell = block[1:2]
                row = jnp.floor(cell * (1.0 / TC))
                col = cell - row * TC
                rights.append(jnp.where(row_iota == packed_row(row)[None], one, zero).reshape(TR, LANES))
                lefts.append(
                    jnp.where(iota == packed_row(col)[None], packed_row(block[0:1])[None], zero).reshape(LANES, LANES)
                )
            left, right = jnp.concatenate(lefts, axis=1), jnp.concatenate(rights, axis=1)
            total = total + lax.dot_general(left, right, NT, preferred_element_type=F32)
        return total

    tile = lax.fori_loop(0, depth, raster, jnp.zeros((TC, TR), F32))
    part[...] = tile.T.reshape(reps, quarter, TC)

    for k in range(1, reps):
        peer = lax.rem(r + k, reps)
        pltpu.make_async_remote_copy(
            src_ref=part.at[peer],
            dst_ref=gathered.at[k - 1],
            send_sem=part_send_sem,
            recv_sem=part_recv_sem,
            device_id={"files": f, "rep": peer},
            device_id_type=MESH,
        ).start()
    pltpu.make_async_copy(gathered, gathered, part_recv_sem).wait()
    out = part[r]
    for k in range(reps - 1):
        out = out + gathered[k]
    out_ref[...] = out

    sent = send.at[pl.ds(0, 2 * (files - 1))]
    pltpu.make_async_copy(sent, sent, send_sem).wait()
    pltpu.make_async_copy(gathered, gathered, part_send_sem).wait()


def solution(mesh):
    files, reps = mesh.shape["files"], mesh.shape["rep"]
    depth = DEPTH if files % (2 * DEPTH) == 0 else 2

    def per_device(tile_id, pix_row, pix_col, point_value):
        count = tile_id.shape[0]
        blocks = count // LANES
        shaped = [a.reshape(blocks, LANES) for a in (tile_id, pix_row, pix_col, point_value)]
        out = pl.pallas_call(
            functools.partial(kernel, files, reps),
            out_shape=jax.ShapeDtypeStruct((TR // reps, TC), F32),
            in_specs=[pl.BlockSpec(memory_space=pltpu.HBM)] * 4,
            out_specs=pl.BlockSpec(memory_space=pltpu.VMEM),
            scratch_shapes=[
                pltpu.VMEM((3, blocks, LANES), jnp.int32),
                pltpu.VMEM((blocks, LANES), BF),
                pltpu.VMEM((3, blocks, LANES), F32),
                pltpu.VMEM((2 * files, CAP), F32),
                pltpu.VMEM((depth, files // depth, 2, CAP), F32),
                pltpu.VMEM((reps, TR // reps, TC), F32),
                pltpu.VMEM((reps - 1, TR // reps, TC), F32),
                pltpu.SemaphoreType.DMA((2,)),
                pltpu.SemaphoreType.DMA,
                pltpu.SemaphoreType.DMA((depth,)),
                pltpu.SemaphoreType.REGULAR((depth,)),
                pltpu.SemaphoreType.DMA,
                pltpu.SemaphoreType.DMA,
            ],
            compiler_params=pltpu.CompilerParams(
                collective_id=0, has_side_effects=True, vmem_limit_bytes=VMEM
            ),
        )(*[pltpu.with_memory_space_constraint(a, pltpu.HBM) for a in shaped])
        return out[None]

    spec = P(("files", "rep"))
    return jax.shard_map(
        per_device,
        mesh=mesh,
        in_specs=(spec, spec, spec, spec),
        out_specs=P("files", "rep", None),
        check_vma=False,
    )
```

```python
import functools

import jax
import jax.numpy as jnp
from jax import lax
from jax.experimental import pallas as pl
from jax.experimental.pallas import tpu as pltpu
from jax.sharding import PartitionSpec as P

TC = 128
TR = 32
CAP = 128
LANES = 128
SUB = 16
DEPTH = 8
RASTER = 8
GROUP = 32
VMEM = 8 << 20
MESH = pl.DeviceIdType.MESH
BF = jnp.bfloat16
F32 = jnp.float32
NT = (((1,), (1,)), ((), ()))


def packed_row(row):
    return jnp.broadcast_to(row, (SUB, LANES)).astype(BF)


def packed_iota(rows):
    count = lax.broadcasted_iota(jnp.int32, (rows // SUB, SUB, LANES), 0) * SUB
    return (count + lax.broadcasted_iota(jnp.int32, (rows // SUB, SUB, LANES), 1)).astype(F32).astype(BF)


def kernel(
    files,
    reps,
    tid_hbm,
    row_hbm,
    col_hbm,
    val_hbm,
    out_ref,
    ids_in,
    val_in,
    points,
    send,
    recv,
    part,
    gathered,
    in_sem,
    send_sem,
    recv_sem,
    above,
    part_send_sem,
    part_recv_sem,
):
    f = lax.axis_index("files")
    r = lax.axis_index("rep")
    depth, line = recv.shape[:2]
    z = lax.rem(f // 2, depth)
    i = f // (2 * depth) * 2 + lax.rem(f, 2)

    def file_on(place, level):
        return place // 2 * depth * 2 + place % 2 + level * 2

    blocks = val_in.shape[0]
    quarter = TR // reps

    loads = [
        pltpu.make_async_copy(tid_hbm, ids_in.at[0], in_sem.at[0]),
        pltpu.make_async_copy(row_hbm, ids_in.at[1], in_sem.at[0]),
        pltpu.make_async_copy(col_hbm, ids_in.at[2], in_sem.at[0]),
        pltpu.make_async_copy(val_hbm, val_in, in_sem.at[1]),
    ]
    for load in loads:
        load.start()

    barrier = pltpu.get_barrier_semaphore()
    def tell(semaphore, peer):
        pl.semaphore_signal(semaphore, inc=1, device_id={"files": peer, "rep": r}, device_id_type=MESH)

    for place in range(line):
        pl.when(i != place)(functools.partial(tell, barrier, file_on(place, z)))
    for k in range(1, reps):
        pl.semaphore_signal(
            barrier, inc=1, device_id={"files": f, "rep": lax.rem(r + k, reps)}, device_id_type=MESH
        )

    def greet(level, _):
        for place in range(line):
            tell(barrier, file_on(place, level))
        return 0

    lax.fori_loop(z + 1, depth, greet, 0)

    pltpu.make_async_copy(ids_in, ids_in, in_sem.at[0]).wait()
    loads[3].wait()
    row = ids_in[1]
    power = jnp.left_shift(1, row & 15).astype(F32) * jnp.where(row >= 16, 65536.0, 1.0)
    points[0] = ids_in[0].astype(F32)
    points[1] = (ids_in[2] + TC).astype(F32) * power
    points[2] = val_in[...].astype(F32)

    iota = packed_iota(LANES)
    one, zero = jnp.ones((), BF), jnp.zeros((), BF)

    def tally(b, total):
        tid = packed_row(points[0, pl.ds(b, 1), :])
        return total + jnp.where(iota == tid[None], one, zero)

    total = lax.fori_loop(0, blocks, tally, jnp.zeros((LANES // SUB, SUB, LANES), BF), unroll=8)
    earlier = jnp.where(
        lax.broadcasted_iota(jnp.int32, (LANES, LANES), 0) < lax.broadcasted_iota(jnp.int32, (LANES, LANES), 1),
        1.0,
        0.0,
    ).astype(BF)
    before = jnp.dot(total.reshape(LANES, LANES), earlier, preferred_element_type=F32)
    before = before.astype(BF).reshape(LANES // SUB, SUB, LANES)

    def place(b, carry):
        before, packed = carry
        lefts, rights = [], []
        for step in range(group):
            at = b * group + step
            hit = iota == packed_row(points[0, pl.ds(at, 1), :])[None]
            slot = jnp.sum(jnp.where(hit, before, zero), axis=0)
            slot = jnp.sum(slot.astype(F32), axis=0, keepdims=True)
            count = jnp.where(hit, one, zero)
            before = before + count
            lefts.append(count.reshape(LANES, LANES))
            here = iota == packed_row(slot)[None]
            rights.append(
                jnp.concatenate(
                    [
                        jnp.where(here, packed_row(points[plane, pl.ds(at, 1), :])[None], zero).reshape(CAP, LANES)
                        for plane in (1, 2)
                    ],
                    axis=0,
                )
            )
        left, right = jnp.concatenate(lefts, axis=1), jnp.concatenate(rights, axis=1)
        return before, packed + lax.dot_general(left, right, NT, preferred_element_type=F32)

    group = min(GROUP, blocks)
    _, packed = lax.fori_loop(0, blocks // group, place, (before, jnp.zeros((LANES, 2 * CAP), F32)))
    code, row = packed[:files, :CAP], jnp.zeros((files, CAP), F32)
    for bit in (16, 8, 4, 2, 1):
        high = code >= 128.0 * 2.0**bit
        code = jnp.where(high, code * 2.0**-bit, code)
        row = row + jnp.where(high, float(bit), 0.0)
    send[pl.ds(0, files, stride=2), :] = packed[:files, CAP:]
    send[pl.ds(1, files, stride=2), :] = row * TC + (code - TC)

    own = pltpu.make_async_copy(send.at[pl.ds(2 * f, 2)], recv.at[z, i], recv_sem.at[z])
    own.start()

    def scatter(level, skip):
        for place in range(line):
            peer = file_on(place, level)

            def start(peer=peer):
                pltpu.make_async_remote_copy(
                    src_ref=send.at[pl.ds(2 * peer, 2)],
                    dst_ref=recv.at[z, i],
                    send_sem=send_sem,
                    recv_sem=recv_sem.at[z],
                    device_id={"files": peer, "rep": r},
                    device_id_type=MESH,
                ).start()

            if skip:
                pl.when(i != place)(start)
            else:
                start()

    pl.semaphore_wait(barrier, line - 1 + reps - 1 + z * line)

    def lower(level, _):
        scatter(level, False)
        return 0

    def announce(level, _):
        tell(above.at[z], f + (level - z) * 2)
        return 0

    lax.fori_loop(0, z, announce, 0)
    lax.fori_loop(0, z, lower, 0)
    scatter(z, True)

    def upper(level, _):
        pl.semaphore_wait(above.at[level], 1)
        scatter(level, False)
        return 0

    lax.fori_loop(z + 1, depth, upper, 0)

    row_iota = packed_iota(TR)

    def raster(step, total):
        level = jnp.where(z < depth // 2, step, depth - 1 - step)
        landed = recv.at[level]
        pltpu.make_async_copy(landed, landed, recv_sem.at[level]).wait()
        for group in range(0, line, RASTER):
            lefts, rights = [], []
            for source in range(group, min(group + RASTER, line)):
                block = recv[level, source]
                cell = block[1:2]
                row = jnp.floor(cell * (1.0 / TC))
                col = cell - row * TC
                rights.append(jnp.where(row_iota == packed_row(row)[None], one, zero).reshape(TR, LANES))
                lefts.append(
                    jnp.where(iota == packed_row(col)[None], packed_row(block[0:1])[None], zero).reshape(LANES, LANES)
                )
            left, right = jnp.concatenate(lefts, axis=1), jnp.concatenate(rights, axis=1)
            total = total + lax.dot_general(right, left, NT, preferred_element_type=F32)
        return total

    tile = lax.fori_loop(0, depth, raster, jnp.zeros((TR, TC), F32))
    part[...] = tile.reshape(reps, quarter, TC)

    for k in range(1, reps):
        peer = lax.rem(r + k, reps)
        pltpu.make_async_remote_copy(
            src_ref=part.at[peer],
            dst_ref=gathered.at[k - 1],
            send_sem=part_send_sem,
            recv_sem=part_recv_sem,
            device_id={"files": f, "rep": peer},
            device_id_type=MESH,
        ).start()
    pltpu.make_async_copy(gathered, gathered, part_recv_sem).wait()
    out = part[r]
    for k in range(reps - 1):
        out = out + gathered[k]
    out_ref[...] = out

    sent = send.at[pl.ds(0, 2 * (files - 1))]
    pltpu.make_async_copy(sent, sent, send_sem).wait()
    pltpu.make_async_copy(gathered, gathered, part_send_sem).wait()


def solution(mesh):
    files, reps = mesh.shape["files"], mesh.shape["rep"]
    depth = DEPTH if files % (2 * DEPTH) == 0 else 2

    def per_device(tile_id, pix_row, pix_col, point_value):
        count = tile_id.shape[0]
        blocks = count // LANES
        shaped = [a.reshape(blocks, LANES) for a in (tile_id, pix_row, pix_col, point_value)]
        out = pl.pallas_call(
            functools.partial(kernel, files, reps),
            out_shape=jax.ShapeDtypeStruct((TR // reps, TC), F32),
            in_specs=[pl.BlockSpec(memory_space=pltpu.HBM)] * 4,
            out_specs=pl.BlockSpec(memory_space=pltpu.VMEM),
            scratch_shapes=[
                pltpu.VMEM((3, blocks, LANES), jnp.int32),
                pltpu.VMEM((blocks, LANES), BF),
                pltpu.VMEM((3, blocks, LANES), F32),
                pltpu.VMEM((2 * files, CAP), F32),
                pltpu.VMEM((depth, files // depth, 2, CAP), F32),
                pltpu.VMEM((reps, TR // reps, TC), F32),
                pltpu.VMEM((reps - 1, TR // reps, TC), F32),
                pltpu.SemaphoreType.DMA((2,)),
                pltpu.SemaphoreType.DMA,
                pltpu.SemaphoreType.DMA((depth,)),
                pltpu.SemaphoreType.REGULAR((depth,)),
                pltpu.SemaphoreType.DMA,
                pltpu.SemaphoreType.DMA,
            ],
            compiler_params=pltpu.CompilerParams(
                collective_id=0, has_side_effects=True, vmem_limit_bytes=VMEM
            ),
        )(*[pltpu.with_memory_space_constraint(a, pltpu.HBM) for a in shaped])
        return out[None]

    spec = P(("files", "rep"))
    return jax.shard_map(
        per_device,
        mesh=mesh,
        in_specs=(spec, spec, spec, spec),
        out_specs=P("files", "rep", None),
        check_vma=False,
    )
```

```python
import functools

import jax
import jax.numpy as jnp
from jax import lax
from jax.experimental import pallas as pl
from jax.experimental.pallas import tpu as pltpu
from jax.sharding import PartitionSpec as P

TC = 128
TR = 32
CAP = 128
LANES = 128
SUB = 16
DEPTH = 8
RASTER = 8
GROUP = 32
VMEM = 8 << 20
MESH = pl.DeviceIdType.MESH
BF = jnp.bfloat16
F32 = jnp.float32
NT = (((1,), (1,)), ((), ()))


def packed_row(row):
    return jnp.broadcast_to(row, (SUB, LANES)).astype(BF)


def packed_iota(rows):
    count = lax.broadcasted_iota(jnp.int32, (rows // SUB, SUB, LANES), 0) * SUB
    return (count + lax.broadcasted_iota(jnp.int32, (rows // SUB, SUB, LANES), 1)).astype(F32).astype(BF)


def kernel(
    files,
    reps,
    tid_hbm,
    row_hbm,
    col_hbm,
    val_hbm,
    out_ref,
    ids_in,
    val_in,
    points,
    send,
    recv,
    part,
    gathered,
    in_sem,
    send_sem,
    recv_sem,
    above,
    part_recv_sem,
):
    f = lax.axis_index("files")
    r = lax.axis_index("rep")
    depth, line = recv.shape[:2]
    z = lax.rem(f // 2, depth)
    y, core = f // (2 * depth), lax.rem(f, 2)
    i = y * 2 + core

    def file_on(place, level):
        return place // 2 * depth * 2 + place % 2 + level * 2

    half = depth // 2
    blocks = val_in.shape[0]
    quarter = TR // reps

    loads = [
        pltpu.make_async_copy(tid_hbm, ids_in.at[0], in_sem),
        pltpu.make_async_copy(row_hbm, ids_in.at[1], in_sem),
        pltpu.make_async_copy(col_hbm, ids_in.at[2], in_sem),
        pltpu.make_async_copy(val_hbm, val_in, in_sem),
    ]
    for load in loads:
        load.start()

    barrier = pltpu.get_barrier_semaphore()
    def tell(semaphore, peer):
        pl.semaphore_signal(semaphore, inc=1, device_id={"files": peer, "rep": r}, device_id_type=MESH)

    tell(barrier, f + 1 - 2 * core)
    rows = line // 2
    for step in sorted(range(1, rows), key=lambda step: min(step, rows - step)):
        there = y + step
        there = jnp.where(there >= rows, there - rows, there) * (2 * depth) + z * 2
        tell(barrier, there)
        tell(barrier, there + 1)
    for k in range(1, reps):
        pl.semaphore_signal(
            barrier, inc=1, device_id={"files": f, "rep": lax.rem(r + k, reps)}, device_id_type=MESH
        )

    def greet(level, _):
        for place in range(line):
            tell(barrier, file_on(place, level))
        return 0

    lax.fori_loop(z + 1, depth, greet, 0)

    loaded = send.at[pl.ds(0, blocks * 7 // 2)]
    pltpu.make_async_copy(loaded, loaded, in_sem).wait()

    row = ids_in[1]
    power = jnp.left_shift(1, row & 15).astype(F32) * jnp.where(row >= 16, 65536.0, 1.0)
    points[0] = ids_in[0].astype(F32)
    points[1] = (ids_in[2] + TC).astype(F32) * power
    points[2] = val_in[...].astype(F32)

    iota = packed_iota(LANES)
    one, zero = jnp.ones((), BF), jnp.zeros((), BF)

    def tally(b, total):
        tid = packed_row(points[0, pl.ds(b, 1), :])
        return total + jnp.where(iota == tid[None], one, zero)

    total = lax.fori_loop(0, blocks, tally, jnp.zeros((LANES // SUB, SUB, LANES), BF), unroll=min(32, blocks))
    earlier = jnp.where(
        lax.broadcasted_iota(jnp.int32, (LANES, LANES), 0) < lax.broadcasted_iota(jnp.int32, (LANES, LANES), 1),
        1.0,
        0.0,
    ).astype(BF)
    before = jnp.dot(total.reshape(LANES, LANES), earlier, preferred_element_type=F32)
    before = before.astype(BF).reshape(LANES // SUB, SUB, LANES)

    def place(b, carry):
        before, packed = carry
        lefts, rights = [], []
        for step in range(group):
            at = b * group + step
            hit = iota == packed_row(points[0, pl.ds(at, 1), :])[None]
            slot = jnp.sum(jnp.where(hit, before, zero), axis=0)
            slot = jnp.sum(slot.astype(F32), axis=0, keepdims=True)
            count = jnp.where(hit, one, zero)
            before = before + count
            lefts.append(count.reshape(LANES, LANES))
            here = iota == packed_row(slot)[None]
            rights.append(
                jnp.concatenate(
                    [
                        jnp.where(here, packed_row(points[plane, pl.ds(at, 1), :])[None], zero).reshape(CAP, LANES)
                        for plane in (1, 2)
                    ],
                    axis=0,
                )
            )
        left, right = jnp.concatenate(lefts, axis=1), jnp.concatenate(rights, axis=1)
        return before, packed + lax.dot_general(left, right, NT, preferred_element_type=F32)

    group = min(GROUP, blocks)
    _, packed = lax.fori_loop(0, blocks // group, place, (before, jnp.zeros((LANES, 2 * CAP), F32)))
    code, row = packed[:files, :CAP], jnp.zeros((files, CAP), F32)
    for bit in (16, 8, 4, 2, 1):
        high = code >= 128.0 * 2.0**bit
        code = jnp.where(high, code * 2.0**-bit, code)
        row = row + jnp.where(high, float(bit), 0.0)
    send[pl.ds(0, files, stride=2), :] = packed[:files, CAP:]
    send[pl.ds(1, files, stride=2), :] = row * TC + (code - TC)

    own = pltpu.make_async_copy(send.at[pl.ds(2 * f, 2)], recv.at[z, i], recv_sem.at[jnp.maximum(z - half + 1, 0)])
    own.start()

    def scatter(level, skip):
        for place in range(line):
            peer = file_on(place, level)

            def start(peer=peer):
                pltpu.make_async_remote_copy(
                    src_ref=send.at[pl.ds(2 * peer, 2)],
                    dst_ref=recv.at[z, i],
                    send_sem=send_sem,
                    recv_sem=recv_sem.at[jnp.maximum(z - half + 1, 0)],
                    device_id={"files": peer, "rep": r},
                    device_id_type=MESH,
                ).start()

            if skip:
                pl.when(i != place)(start)
            else:
                start()

    pl.semaphore_wait(barrier, line - 1 + reps - 1 + z * line)

    def lower(level, _):
        scatter(level, False)
        return 0

    def announce(level, _):
        tell(above.at[jnp.where(z < half, 0, 1 + jnp.maximum(z - half, 0) // 2)], f + (level - z) * 2)
        return 0

    @pl.when(z > 0)
    def _():
        scatter(0, False)

    lax.fori_loop(0, z, announce, 0)
    lax.fori_loop(1, z, lower, 0)
    scatter(z, True)

    def upper(level, _):
        scatter(level, False)
        return 0

    for group, (start, stop) in enumerate([(1, half)] + [(k, min(k + 2, depth)) for k in range(half, depth, 2)]):
        base = jnp.maximum(z + 1, start)

        def heard(group=group, stop=stop, base=base):
            pl.semaphore_wait(above.at[group], stop - base)
            lax.fori_loop(base, stop, upper, 0)

        pl.when(base < stop)(heard)

    row_iota = packed_iota(TR)

    def raster(step, total):
        level = jnp.where(z < half, step, depth - 1 - step)
        landed, lower_half = recv.at[level], recv.at[pl.ds(0, half)]
        alone = pltpu.make_async_copy(landed, landed, recv_sem.at[jnp.maximum(level - half + 1, 0)])
        pl.when(level >= half)(alone.wait)
        together = pltpu.make_async_copy(lower_half, lower_half, recv_sem.at[0])
        pl.when(level == jnp.where(z < half, 0, half - 1))(together.wait)
        for group in range(0, line, RASTER):
            lefts, rights = [], []
            for source in range(group, min(group + RASTER, line)):
                block = recv[level, source]
                cell = block[1:2]
                row = jnp.floor(cell * (1.0 / TC))
                col = cell - row * TC
                rights.append(jnp.where(row_iota == packed_row(row)[None], one, zero).reshape(TR, LANES))
                lefts.append(
                    jnp.where(iota == packed_row(col)[None], packed_row(block[0:1])[None], zero).reshape(LANES, LANES)
                )
            left, right = jnp.concatenate(lefts, axis=1), jnp.concatenate(rights, axis=1)
            total = total + lax.dot_general(right, left, NT, preferred_element_type=F32)
        return total

    tile = lax.fori_loop(0, depth, raster, jnp.zeros((TR, TC), F32))
    part[...] = tile.reshape(reps, quarter, TC)

    for k in sorted(range(1, reps), key=lambda k: -min(k, reps - k)):
        peer = lax.rem(r + k, reps)
        pltpu.make_async_remote_copy(
            src_ref=part.at[peer],
            dst_ref=gathered.at[k - 1],
            send_sem=in_sem,
            recv_sem=part_recv_sem,
            device_id={"files": f, "rep": peer},
            device_id_type=MESH,
        ).start()
    pltpu.make_async_copy(gathered, gathered, part_recv_sem).wait()
    out = part[r]
    for k in range(reps - 1):
        out = out + gathered[k]
    out_ref[...] = out

    sent = send.at[pl.ds(0, 2 * (files - 1))]
    pltpu.make_async_copy(sent, sent, send_sem).wait()
    pltpu.make_async_copy(gathered, gathered, in_sem).wait()


def solution(mesh):
    files, reps = mesh.shape["files"], mesh.shape["rep"]
    depth = DEPTH if files % (2 * DEPTH) == 0 else 2

    def per_device(tile_id, pix_row, pix_col, point_value):
        count = tile_id.shape[0]
        blocks = count // LANES
        shaped = [a.reshape(blocks, LANES) for a in (tile_id, pix_row, pix_col, point_value)]
        out = pl.pallas_call(
            functools.partial(kernel, files, reps),
            out_shape=jax.ShapeDtypeStruct((TR // reps, TC), F32),
            in_specs=[pl.BlockSpec(memory_space=pltpu.HBM)] * 4,
            out_specs=pl.BlockSpec(memory_space=pltpu.VMEM),
            scratch_shapes=[
                pltpu.VMEM((3, blocks, LANES), jnp.int32),
                pltpu.VMEM((blocks, LANES), BF),
                pltpu.VMEM((3, blocks, LANES), F32),
                pltpu.VMEM((2 * files + SUB, CAP), F32),
                pltpu.VMEM((depth, files // depth, 2, CAP), F32),
                pltpu.VMEM((reps, TR // reps, TC), F32),
                pltpu.VMEM((reps - 1, TR // reps, TC), F32),
                pltpu.SemaphoreType.DMA,
                pltpu.SemaphoreType.DMA,
                pltpu.SemaphoreType.DMA((depth - depth // 2 + 1,)),
                pltpu.SemaphoreType.REGULAR((2 + (depth - depth // 2 - 1) // 2,)),
                pltpu.SemaphoreType.DMA,
            ],
            compiler_params=pltpu.CompilerParams(
                collective_id=0, has_side_effects=True, vmem_limit_bytes=VMEM
            ),
        )(*[pltpu.with_memory_space_constraint(a, pltpu.HBM) for a in shaped])
        return out[None]

    spec = P(("files", "rep"))
    return jax.shard_map(
        per_device,
        mesh=mesh,
        in_specs=(spec, spec, spec, spec),
        out_specs=P("files", "rep", None),
        check_vma=False,
    )
```

```python
import functools

import jax
import jax.numpy as jnp
from jax import lax
from jax.experimental import pallas as pl
from jax.experimental.pallas import tpu as pltpu
from jax.sharding import PartitionSpec as P

TC = 128
TR = 32
CAP = 128
LANES = 128
SUB = 16
DEPTH = 8
RASTER = 8
GROUP = 32
VMEM = 8 << 20
MESH = pl.DeviceIdType.MESH
BF = jnp.bfloat16
F32 = jnp.float32
NT = (((1,), (1,)), ((), ()))


def packed_row(row):
    return jnp.broadcast_to(row, (SUB, LANES)).astype(BF)


def packed_iota(rows):
    count = lax.broadcasted_iota(jnp.int32, (rows // SUB, SUB, LANES), 0) * SUB
    return (count + lax.broadcasted_iota(jnp.int32, (rows // SUB, SUB, LANES), 1)).astype(F32).astype(BF)


def kernel(
    files,
    reps,
    tid_hbm,
    row_hbm,
    col_hbm,
    val_hbm,
    out_ref,
    ids_in,
    val_in,
    points,
    send,
    recv,
    part,
    gathered,
    in_sem,
    send_sem,
    recv_sem,
    above,
    part_recv_sem,
):
    f = lax.axis_index("files")
    r = lax.axis_index("rep")
    depth, line = recv.shape[:2]
    z = lax.rem(f // 2, depth)
    y, core = f // (2 * depth), lax.rem(f, 2)
    i = y * 2 + core

    def file_on(place, level):
        return place // 2 * depth * 2 + place % 2 + level * 2

    half = depth // 2
    blocks = val_in.shape[0]
    quarter = TR // reps

    loads = [
        pltpu.make_async_copy(tid_hbm, ids_in.at[0], in_sem),
        pltpu.make_async_copy(row_hbm, ids_in.at[1], in_sem),
        pltpu.make_async_copy(col_hbm, ids_in.at[2], in_sem),
        pltpu.make_async_copy(val_hbm, val_in, in_sem),
    ]
    for load in loads:
        load.start()

    barrier = pltpu.get_barrier_semaphore()
    def tell(semaphore, peer):
        pl.semaphore_signal(semaphore, inc=1, device_id={"files": peer, "rep": r}, device_id_type=MESH)

    for k in range(1, reps):
        pl.semaphore_signal(
            barrier, inc=1, device_id={"files": f, "rep": lax.rem(r + k, reps)}, device_id_type=MESH
        )

    tell(barrier, f + 1 - 2 * core)
    rows = line // 2
    for step in sorted(range(1, rows), key=lambda step: min(step, rows - step)):
        there = y + step
        there = jnp.where(there >= rows, there - rows, there) * (2 * depth) + z * 2
        tell(barrier, there)
        tell(barrier, there + 1)

    def greet(level, _):
        for place in range(line):
            tell(barrier, file_on(place, level))
        return 0

    lax.fori_loop(z + 1, depth, greet, 0)

    loaded = send.at[pl.ds(0, blocks * 7 // 2)]
    pltpu.make_async_copy(loaded, loaded, in_sem).wait()

    row = ids_in[1]
    power = jnp.left_shift(1, row & 15).astype(F32) * jnp.where(row >= 16, 65536.0, 1.0)
    points[0] = ids_in[0].astype(F32)
    points[1] = (ids_in[2] + TC).astype(F32) * power
    points[2] = val_in[...].astype(F32)

    iota = packed_iota(LANES)
    one, zero = jnp.ones((), BF), jnp.zeros((), BF)

    def tally(b, total):
        tid = packed_row(points[0, pl.ds(b, 1), :])
        return total + jnp.where(iota == tid[None], one, zero)

    total = lax.fori_loop(0, blocks, tally, jnp.zeros((LANES // SUB, SUB, LANES), BF), unroll=min(32, blocks))
    earlier = jnp.where(
        lax.broadcasted_iota(jnp.int32, (LANES, LANES), 0) < lax.broadcasted_iota(jnp.int32, (LANES, LANES), 1),
        1.0,
        0.0,
    ).astype(BF)
    before = jnp.dot(total.reshape(LANES, LANES), earlier, preferred_element_type=F32)
    before = before.astype(BF).reshape(LANES // SUB, SUB, LANES)

    def place(b, carry):
        before, packed = carry
        lefts, rights = [], []
        for step in range(group):
            at = b * group + step
            hit = iota == packed_row(points[0, pl.ds(at, 1), :])[None]
            slot = jnp.sum(jnp.where(hit, before, zero), axis=0)
            slot = jnp.sum(slot.astype(F32), axis=0, keepdims=True)
            count = jnp.where(hit, one, zero)
            before = before + count
            lefts.append(count.reshape(LANES, LANES))
            here = iota == packed_row(slot)[None]
            rights.append(
                jnp.concatenate(
                    [
                        jnp.where(here, packed_row(points[plane, pl.ds(at, 1), :])[None], zero).reshape(CAP, LANES)
                        for plane in (1, 2)
                    ],
                    axis=0,
                )
            )
        left, right = jnp.concatenate(lefts, axis=1), jnp.concatenate(rights, axis=1)
        return before, packed + lax.dot_general(left, right, NT, preferred_element_type=F32)

    group = min(GROUP, blocks)
    _, packed = lax.fori_loop(0, blocks // group, place, (before, jnp.zeros((LANES, 2 * CAP), F32)))
    code, row = packed[:files, :CAP], jnp.zeros((files, CAP), F32)
    for bit in (16, 8, 4, 2, 1):
        high = code >= 128.0 * 2.0**bit
        code = jnp.where(high, code * 2.0**-bit, code)
        row = row + jnp.where(high, float(bit), 0.0)
    send[pl.ds(0, files, stride=2), :] = packed[:files, CAP:]
    send[pl.ds(1, files, stride=2), :] = row * TC + (code - TC)

    own = pltpu.make_async_copy(send.at[pl.ds(2 * f, 2)], recv.at[z, i], recv_sem.at[jnp.maximum(z - half + 1, 0)])
    own.start()

    def scatter(level, skip):
        for place in range(line):
            peer = file_on(place, level)

            def start(peer=peer):
                pltpu.make_async_remote_copy(
                    src_ref=send.at[pl.ds(2 * peer, 2)],
                    dst_ref=recv.at[z, i],
                    send_sem=send_sem,
                    recv_sem=recv_sem.at[jnp.maximum(z - half + 1, 0)],
                    device_id={"files": peer, "rep": r},
                    device_id_type=MESH,
                ).start()

            if skip:
                pl.when(i != place)(start)
            else:
                start()

    pl.semaphore_wait(barrier, line - 1 + reps - 1 + z * line)

    def lower(level, _):
        scatter(level, False)
        return 0

    def announce(level, _):
        tell(above.at[jnp.where(z < half, 0, 1 + jnp.maximum(z - half, 0) // 2)], f + (level - z) * 2)
        return 0

    @pl.when(z > 0)
    def _():
        scatter(0, False)

    lax.fori_loop(0, z, announce, 0)
    lax.fori_loop(1, z, lower, 0)
    scatter(z, True)

    def upper(level, _):
        scatter(level, False)
        return 0

    for group, (start, stop) in enumerate([(1, half)] + [(k, min(k + 2, depth)) for k in range(half, depth, 2)]):
        base = jnp.maximum(z + 1, start)

        def heard(group=group, stop=stop, base=base):
            pl.semaphore_wait(above.at[group], stop - base)
            lax.fori_loop(base, stop, upper, 0)

        pl.when(base < stop)(heard)

    row_iota = packed_iota(TR)

    def raster(step, total):
        level = jnp.where(z < half, step, depth - 1 - step)
        landed, lower_half = recv.at[level], recv.at[pl.ds(0, half)]
        alone = pltpu.make_async_copy(landed, landed, recv_sem.at[jnp.maximum(level - half + 1, 0)])
        pl.when(level >= half)(alone.wait)
        together = pltpu.make_async_copy(lower_half, lower_half, recv_sem.at[0])
        pl.when(level == jnp.where(z < half, 0, half - 1))(together.wait)
        for group in range(0, line, RASTER):
            lefts, rights = [], []
            for source in range(group, min(group + RASTER, line)):
                block = recv[level, source]
                cell = block[1:2]
                row = jnp.floor(cell * (1.0 / TC))
                col = cell - row * TC
                rights.append(jnp.where(row_iota == packed_row(row)[None], one, zero).reshape(TR, LANES))
                lefts.append(
                    jnp.where(iota == packed_row(col)[None], packed_row(block[0:1])[None], zero).reshape(LANES, LANES)
                )
            left, right = jnp.concatenate(lefts, axis=1), jnp.concatenate(rights, axis=1)
            total = total + lax.dot_general(right, left, NT, preferred_element_type=F32)
        return total

    tile = lax.fori_loop(0, depth, raster, jnp.zeros((TR, TC), F32))
    part[...] = tile.reshape(reps, quarter, TC)

    for k in sorted(range(1, reps), key=lambda k: -min(k, reps - k)):
        peer = lax.rem(r + k, reps)
        pltpu.make_async_remote_copy(
            src_ref=part.at[peer],
            dst_ref=gathered.at[k - 1],
            send_sem=in_sem,
            recv_sem=part_recv_sem,
            device_id={"files": f, "rep": peer},
            device_id_type=MESH,
        ).start()
    pltpu.make_async_copy(gathered, gathered, part_recv_sem).wait()
    out = part[r]
    for k in range(reps - 1):
        out = out + gathered[k]
    out_ref[...] = out

    sent = send.at[pl.ds(0, 2 * (files - 1))]
    pltpu.make_async_copy(sent, sent, send_sem).wait()
    pltpu.make_async_copy(gathered, gathered, in_sem).wait()


def solution(mesh):
    files, reps = mesh.shape["files"], mesh.shape["rep"]
    depth = DEPTH if files % (2 * DEPTH) == 0 else 2

    def per_device(tile_id, pix_row, pix_col, point_value):
        count = tile_id.shape[0]
        blocks = count // LANES
        shaped = [a.reshape(blocks, LANES) for a in (tile_id, pix_row, pix_col, point_value)]
        out = pl.pallas_call(
            functools.partial(kernel, files, reps),
            out_shape=jax.ShapeDtypeStruct((TR // reps, TC), F32),
            in_specs=[pl.BlockSpec(memory_space=pltpu.HBM)] * 4,
            out_specs=pl.BlockSpec(memory_space=pltpu.VMEM),
            scratch_shapes=[
                pltpu.VMEM((3, blocks, LANES), jnp.int32),
                pltpu.VMEM((blocks, LANES), BF),
                pltpu.VMEM((3, blocks, LANES), F32),
                pltpu.VMEM((2 * files + SUB, CAP), F32),
                pltpu.VMEM((depth, files // depth, 2, CAP), F32),
                pltpu.VMEM((reps, TR // reps, TC), F32),
                pltpu.VMEM((reps - 1, TR // reps, TC), F32),
                pltpu.SemaphoreType.DMA,
                pltpu.SemaphoreType.DMA,
                pltpu.SemaphoreType.DMA((depth - depth // 2 + 1,)),
                pltpu.SemaphoreType.REGULAR((2 + (depth - depth // 2 - 1) // 2,)),
                pltpu.SemaphoreType.DMA,
            ],
            compiler_params=pltpu.CompilerParams(
                collective_id=0, has_side_effects=True, vmem_limit_bytes=VMEM
            ),
        )(*[pltpu.with_memory_space_constraint(a, pltpu.HBM) for a in shaped])
        return out[None]

    spec = P(("files", "rep"))
    return jax.shard_map(
        per_device,
        mesh=mesh,
        in_specs=(spec, spec, spec, spec),
        out_specs=P("files", "rep", None),
        check_vma=False,
    )
```

```python
import functools

import jax
import jax.numpy as jnp
from jax import lax
from jax.experimental import pallas as pl
from jax.experimental.pallas import tpu as pltpu
from jax.sharding import PartitionSpec as P

TC = 128
TR = 32
CAP = 128
LANES = 128
SUB = 16
DEPTH = 8
RASTER = 16
GROUP = 32
VMEM = 8 << 20
MESH = pl.DeviceIdType.MESH
BF = jnp.bfloat16
F32 = jnp.float32
NT = (((1,), (1,)), ((), ()))


def packed_row(row):
    return jnp.broadcast_to(row, (SUB, LANES)).astype(BF)


def packed_iota(rows):
    count = lax.broadcasted_iota(jnp.int32, (rows // SUB, SUB, LANES), 0) * SUB
    return (count + lax.broadcasted_iota(jnp.int32, (rows // SUB, SUB, LANES), 1)).astype(F32).astype(BF)


def kernel(
    files,
    reps,
    tid_hbm,
    row_hbm,
    col_hbm,
    val_hbm,
    out_ref,
    ids_in,
    val_in,
    points,
    send,
    recv,
    part,
    gathered,
    in_sem,
    send_sem,
    recv_sem,
    above,
    part_recv_sem,
):
    f = lax.axis_index("files")
    r = lax.axis_index("rep")
    depth, line = recv.shape[:2]
    z = lax.rem(f // 2, depth)
    y, core = f // (2 * depth), lax.rem(f, 2)
    i = y * 2 + core

    def file_on(place, level):
        return place // 2 * depth * 2 + place % 2 + level * 2

    half = depth // 2
    blocks = val_in.shape[0]
    quarter = TR // reps

    loads = [
        pltpu.make_async_copy(tid_hbm, ids_in.at[0], in_sem),
        pltpu.make_async_copy(row_hbm, ids_in.at[1], in_sem),
        pltpu.make_async_copy(col_hbm, ids_in.at[2], in_sem),
        pltpu.make_async_copy(val_hbm, val_in, in_sem),
    ]
    for load in loads:
        load.start()

    barrier = pltpu.get_barrier_semaphore()
    def tell(semaphore, peer):
        pl.semaphore_signal(semaphore, inc=1, device_id={"files": peer, "rep": r}, device_id_type=MESH)

    tell(barrier, f + 1 - 2 * core)
    rows = line // 2
    for step in sorted(range(1, rows), key=lambda step: min(step, rows - step)):
        there = y + step
        there = jnp.where(there >= rows, there - rows, there) * (2 * depth) + z * 2
        tell(barrier, there)
        tell(barrier, there + 1)
    for k in range(1, reps):
        pl.semaphore_signal(
            barrier, inc=1, device_id={"files": f, "rep": lax.rem(r + k, reps)}, device_id_type=MESH
        )

    def greet(level, _):
        for place in range(line):
            tell(barrier, file_on(place, level))
        return 0

    lax.fori_loop(z + 1, depth, greet, 0)

    loaded = send.at[pl.ds(0, blocks * 7 // 2)]
    pltpu.make_async_copy(loaded, loaded, in_sem).wait()

    row = ids_in[1]
    power = jnp.left_shift(1, row & 15).astype(F32) * jnp.where(row >= 16, 65536.0, 1.0)
    points[0] = ids_in[0].astype(F32)
    points[1] = (ids_in[2] + TC).astype(F32) * power
    points[2] = val_in[...].astype(F32)

    iota = packed_iota(LANES)
    one, zero = jnp.ones((), BF), jnp.zeros((), BF)

    def tally(b, total):
        tid = packed_row(points[0, pl.ds(b, 1), :])
        return total + jnp.where(iota == tid[None], one, zero)

    total = lax.fori_loop(0, blocks, tally, jnp.zeros((LANES // SUB, SUB, LANES), BF), unroll=min(32, blocks))
    earlier = jnp.where(
        lax.broadcasted_iota(jnp.int32, (LANES, LANES), 0) < lax.broadcasted_iota(jnp.int32, (LANES, LANES), 1),
        1.0,
        0.0,
    ).astype(BF)
    before = jnp.dot(total.reshape(LANES, LANES), earlier, preferred_element_type=F32)
    before = before.astype(BF).reshape(LANES // SUB, SUB, LANES)

    def place(b, carry):
        before, packed = carry
        lefts, rights = [], []
        for step in range(group):
            at = b * group + step
            hit = iota == packed_row(points[0, pl.ds(at, 1), :])[None]
            slot = jnp.sum(jnp.where(hit, before, zero), axis=0)
            slot = jnp.sum(slot.astype(F32), axis=0, keepdims=True)
            count = jnp.where(hit, one, zero)
            before = before + count
            lefts.append(count.reshape(LANES, LANES))
            here = iota == packed_row(slot)[None]
            rights.append(
                jnp.concatenate(
                    [
                        jnp.where(here, packed_row(points[plane, pl.ds(at, 1), :])[None], zero).reshape(CAP, LANES)
                        for plane in (1, 2)
                    ],
                    axis=0,
                )
            )
        left, right = jnp.concatenate(lefts, axis=1), jnp.concatenate(rights, axis=1)
        return before, packed + lax.dot_general(left, right, NT, preferred_element_type=F32)

    group = min(GROUP, blocks)
    _, packed = lax.fori_loop(0, blocks // group, place, (before, jnp.zeros((LANES, 2 * CAP), F32)))
    code, row = packed[:files, :CAP], jnp.zeros((files, CAP), F32)
    for bit in (16, 8, 4, 2, 1):
        high = code >= 128.0 * 2.0**bit
        code = jnp.where(high, code * 2.0**-bit, code)
        row = row + jnp.where(high, float(bit), 0.0)
    send[pl.ds(0, files, stride=2), :] = packed[:files, CAP:]
    send[pl.ds(1, files, stride=2), :] = row * TC + (code - TC)

    own = pltpu.make_async_copy(send.at[pl.ds(2 * f, 2)], recv.at[z, i], recv_sem.at[jnp.maximum(z - half + 1, 0)])
    own.start()

    def scatter(level, skip):
        for place in range(line):
            peer = file_on(place, level)

            def start(peer=peer):
                pltpu.make_async_remote_copy(
                    src_ref=send.at[pl.ds(2 * peer, 2)],
                    dst_ref=recv.at[z, i],
                    send_sem=send_sem,
                    recv_sem=recv_sem.at[jnp.maximum(z - half + 1, 0)],
                    device_id={"files": peer, "rep": r},
                    device_id_type=MESH,
                ).start()

            if skip:
                pl.when(i != place)(start)
            else:
                start()

    pl.semaphore_wait(barrier, line - 1 + reps - 1 + z * line)

    def lower(level, _):
        scatter(level, False)
        return 0

    def announce(level, _):
        tell(above.at[jnp.where(z < half, 0, 1 + jnp.maximum(z - half, 0) // 2)], f + (level - z) * 2)
        return 0

    @pl.when(z > 0)
    def _():
        scatter(0, False)

    lax.fori_loop(0, z, announce, 0)
    lax.fori_loop(1, z, lower, 0)
    scatter(z, True)

    def upper(level, _):
        scatter(level, False)
        return 0

    for group, (start, stop) in enumerate([(1, half)] + [(k, min(k + 2, depth)) for k in range(half, depth, 2)]):
        base = jnp.maximum(z + 1, start)

        def heard(group=group, stop=stop, base=base):
            pl.semaphore_wait(above.at[group], stop - base)
            lax.fori_loop(base, stop, upper, 0)

        pl.when(base < stop)(heard)

    row_iota = packed_iota(TR)

    def raster(step, total):
        level = jnp.where(z < half, step, depth - 1 - step)
        landed, lower_half = recv.at[level], recv.at[pl.ds(0, half)]
        alone = pltpu.make_async_copy(landed, landed, recv_sem.at[jnp.maximum(level - half + 1, 0)])
        pl.when(level >= half)(alone.wait)
        together = pltpu.make_async_copy(lower_half, lower_half, recv_sem.at[0])
        pl.when(level == jnp.where(z < half, 0, half - 1))(together.wait)
        for group in range(0, line, RASTER):
            lefts, rights = [], []
            for source in range(group, min(group + RASTER, line)):
                block = recv[level, source]
                cell = block[1:2]
                row = jnp.floor(cell * (1.0 / TC))
                col = cell - row * TC
                rights.append(jnp.where(row_iota == packed_row(row)[None], one, zero).reshape(TR, LANES))
                lefts.append(
                    jnp.where(iota == packed_row(col)[None], packed_row(block[0:1])[None], zero).reshape(LANES, LANES)
                )
            left, right = jnp.concatenate(lefts, axis=1), jnp.concatenate(rights, axis=1)
            total = total + lax.dot_general(right, left, NT, preferred_element_type=F32)
        return total

    tile = lax.fori_loop(0, depth, raster, jnp.zeros((TR, TC), F32))
    part[...] = tile.reshape(reps, quarter, TC)

    for k in sorted(range(1, reps), key=lambda k: -min(k, reps - k)):
        peer = lax.rem(r + k, reps)
        pltpu.make_async_remote_copy(
            src_ref=part.at[peer],
            dst_ref=gathered.at[k - 1],
            send_sem=in_sem,
            recv_sem=part_recv_sem,
            device_id={"files": f, "rep": peer},
            device_id_type=MESH,
        ).start()
    pltpu.make_async_copy(gathered, gathered, part_recv_sem).wait()
    out = part[r]
    for k in range(reps - 1):
        out = out + gathered[k]
    out_ref[...] = out

    sent = send.at[pl.ds(0, 2 * (files - 1))]
    pltpu.make_async_copy(sent, sent, send_sem).wait()
    pltpu.make_async_copy(gathered, gathered, in_sem).wait()


def solution(mesh):
    files, reps = mesh.shape["files"], mesh.shape["rep"]
    depth = DEPTH if files % (2 * DEPTH) == 0 else 2

    def per_device(tile_id, pix_row, pix_col, point_value):
        count = tile_id.shape[0]
        blocks = count // LANES
        shaped = [a.reshape(blocks, LANES) for a in (tile_id, pix_row, pix_col, point_value)]
        out = pl.pallas_call(
            functools.partial(kernel, files, reps),
            out_shape=jax.ShapeDtypeStruct((TR // reps, TC), F32),
            in_specs=[pl.BlockSpec(memory_space=pltpu.HBM)] * 4,
            out_specs=pl.BlockSpec(memory_space=pltpu.VMEM),
            scratch_shapes=[
                pltpu.VMEM((3, blocks, LANES), jnp.int32),
                pltpu.VMEM((blocks, LANES), BF),
                pltpu.VMEM((3, blocks, LANES), F32),
                pltpu.VMEM((2 * files + SUB, CAP), F32),
                pltpu.VMEM((depth, files // depth, 2, CAP), F32),
                pltpu.VMEM((reps, TR // reps, TC), F32),
                pltpu.VMEM((reps - 1, TR // reps, TC), F32),
                pltpu.SemaphoreType.DMA,
                pltpu.SemaphoreType.DMA,
                pltpu.SemaphoreType.DMA((depth - depth // 2 + 1,)),
                pltpu.SemaphoreType.REGULAR((2 + (depth - depth // 2 - 1) // 2,)),
                pltpu.SemaphoreType.DMA,
            ],
            compiler_params=pltpu.CompilerParams(
                collective_id=0, has_side_effects=True, vmem_limit_bytes=VMEM
            ),
        )(*[pltpu.with_memory_space_constraint(a, pltpu.HBM) for a in shaped])
        return out[None]

    spec = P(("files", "rep"))
    return jax.shard_map(
        per_device,
        mesh=mesh,
        in_specs=(spec, spec, spec, spec),
        out_specs=P("files", "rep", None),
        check_vma=False,
    )
```
